256 devices in a mesh: node: 256 (over z, x, y, core).
Axes of the slice: x: 4, y: 4, z: 8, core: 2. Of those that a mesh axis runs over, the one named last changes fastest.
Arguments:
- round_index: int32 [1], replicated, may hold values from 0 to 63
- sample_ids: int32 [256, 8], P('node'), may hold values from 0 to 3
- token_pool: bfloat16 [256, 4, 64, 512], P('node'), may hold values from -20 to 20
- cotangent_pool: bfloat16 [256, 4, 64, 512], P('node'), may hold values from -6 to 6
- weights: bfloat16 [256, 4, 512, 512], P('node'), may hold values from -12 to 12
- residue: bfloat16 [256, 4, 512, 512], P('node'), may hold values from -6 to 6
Outputs:
- new_weights: bfloat16 [256, 4, 512, 512], P('node')
- new_residue: bfloat16 [256, 4, 512, 512], P('node')
- grad_rms: float32 [], replicated
The draws below stay inside these ranges and needn't reach their ends.
All inputs are finite; a program needn't handle non-finite values.
Results may differ from the reference program's by a relative error of at most 0.0065.
Values may be sent and summed in bfloat16 or wider, within the bound.
No kernel may reach another device: no remote copies, remote signals or barrier semaphores. Data moves between devices by JAX's collectives and lax.ppermute only.
A program may use at most 128 MiB of HBM per device.

```python
import jax
import jax.numpy as jnp
from jax import lax

HEAD_DIM = 64
D = 512
SEQ = 64
BATCH = 8
POOL = 4
NODES = 256
N_NODE = 256


def draw_weights(key, part):
    shape_all = (NODES, 4, D, D)
    drawn = jax.random.normal(key, shape_all, jnp.float32)
    return jnp.clip(drawn, -12.0, 12.0).astype(jnp.bfloat16)


def draw_token_pool(key, part):
    shape_all = (NODES, POOL, SEQ, D)
    drawn = jax.random.normal(key, shape_all, jnp.float32)
    return jnp.clip(drawn, -20.0, 20.0).astype(jnp.bfloat16)


def draw_cotangent_pool(key, part):
    shape_all = (NODES, POOL, SEQ, D)
    rising = (jnp.arange(NODES, dtype=jnp.float32) / max(NODES - 1, 1)).reshape(NODES, 1, 1, 1)
    drawn = jax.random.normal(key, shape_all, jnp.float32) * 0.5 * jnp.power(3.0, 0.5 * rising)
    return jnp.clip(drawn, -6.0, 6.0).astype(jnp.bfloat16)


def place_ends(values, stream_key, smallest, high):
    longest = values.shape.index(max(values.shape))
    spots = []
    for shift in (0, 1):
        where = [jax.random.randint(jax.random.fold_in(stream_key, axis), (), 0, length) for axis, length in enumerate(values.shape)]
        where[longest] = (where[longest] + shift) % values.shape[longest]
        spots.append(tuple(where))
    return values.at[spots[0]].set(smallest).at[spots[1]].set(high)


def steps_of(stream_key, extent, cuts, smallest, top_value):
    gain, own = 1.0, jax.random.fold_in(stream_key, 6)
    for axis_at, parts in cuts:
        heights = jnp.exp(jax.random.uniform(jax.random.fold_in(own, axis_at), (parts,), jnp.float32, smallest / len(cuts), top_value / len(cuts)))
        gain = gain * jnp.repeat(heights, extent[axis_at] // parts).reshape([-1 if axis == axis_at else 1 for axis in range(len(extent))])
    return gain


def centred(own_key, dims, scale, most, shards=(), held_as=jnp.bfloat16):
    entries = jax.random.normal(own_key, dims, jnp.float32) * scale
    if len(shards) > 0:
        entries = steps_of(own_key, dims, shards, -0.22, 0.18) * entries
    return jnp.clip(entries, min=-most, max=most).astype(held_as)


def setup_inputs(seed: int = 0) -> dict:
    keys = jax.random.split(jax.random.key(seed), 7)
    round_index = jax.random.randint(keys[0], (1,), 0, 64).astype(jnp.int32)
    sample_ids = place_ends(jax.random.randint(keys[1], (NODES, BATCH), 0, POOL), jax.random.fold_in(keys[1], 1), 0, POOL - 1).astype(jnp.int32)
    token_pool = draw_token_pool(jax.random.fold_in(keys[6], 71), 0)
    cotangent_pool = draw_cotangent_pool(jax.random.fold_in(keys[6], 71), 0)
    weights = draw_weights(jax.random.fold_in(keys[6], 71), 0)
    residue = centred(keys[5], (NODES, 4, D, D), 1.0, 6.0, ((0, 256),))
    return {"round_index": round_index, "sample_ids": sample_ids, "token_pool": token_pool, "cotangent_pool": cotangent_pool, "weights": weights, "residue": residue}


epsilon = 1e-06
step_rate = 0.1

def normalize(tokens):
    values = tokens.astype(jnp.float32)
    centered = values - lax.optimization_barrier(jnp.mean(values, -1, keepdims=True))
    variance = lax.optimization_barrier(jnp.mean(centered * centered, -1, keepdims=True))
    return (centered * lax.rsqrt(variance + epsilon)).astype(jnp.bfloat16)

def node_gradient(weights, tokens, cotangent):
    batch_size, seq_len, model_width = tokens.shape
    head_count = model_width // HEAD_DIM
    proj_scale = model_width ** (-0.5)
    head_scale = HEAD_DIM ** (-0.5)
    row_count = batch_size * seq_len
    normed_rows = normalize(tokens).reshape(row_count, model_width)
    grad_rows = cotangent.reshape(row_count, model_width)

    def project(which):
        return (jnp.dot(normed_rows, weights[which], preferred_element_type=jnp.float32) * proj_scale).astype(jnp.bfloat16)

    def to_heads(matrix):
        return matrix.reshape(batch_size, seq_len, head_count, HEAD_DIM).astype(jnp.float32)
    queries = to_heads(project(0))
    key_rows = to_heads(project(1))
    value_rows = to_heads(project(2))
    scores = jnp.einsum('bshe,bthe->bhst', queries, key_rows) * head_scale
    attn_probs = jnp.exp(scores - lax.optimization_barrier(jnp.max(scores, -1, keepdims=True)))
    attn_probs = attn_probs / lax.optimization_barrier(jnp.sum(attn_probs, -1, keepdims=True))
    probs_half = attn_probs.astype(jnp.bfloat16).astype(jnp.float32)
    context = jnp.einsum('bhst,bthe->bshe', probs_half, value_rows).astype(jnp.bfloat16).reshape(row_count, model_width)
    grad_out = jnp.dot(context.T, grad_rows, preferred_element_type=jnp.float32) * proj_scale
    context_grad = (jnp.dot(grad_rows, weights[3].T, preferred_element_type=jnp.float32) * proj_scale).astype(jnp.bfloat16)
    context_heads = to_heads(context_grad)
    probs_grad = jnp.einsum('bshe,bthe->bhst', context_heads, value_rows)
    value_grad = jnp.einsum('bhst,bshe->bthe', probs_half, context_heads).astype(jnp.bfloat16)
    score_grad = (attn_probs * (probs_grad - lax.optimization_barrier(jnp.sum(probs_grad * attn_probs, -1, keepdims=True))) * head_scale).astype(jnp.bfloat16).astype(jnp.float32)
    query_grad = jnp.einsum('bhst,bthe->bshe', score_grad, key_rows).astype(jnp.bfloat16)
    key_grad = jnp.einsum('bhst,bshe->bthe', score_grad, queries).astype(jnp.bfloat16)

    def weight_grad(rows_grad):
        return jnp.dot(normed_rows.T, rows_grad.reshape(row_count, model_width), preferred_element_type=jnp.float32) * proj_scale
    return jnp.stack([weight_grad(query_grad), weight_grad(key_grad), weight_grad(value_grad), grad_out])

def reference(round_index, sample_ids, token_pool, cotangent_pool, weights, residue):

    def per_node(node_index):
        sample_rows = sample_ids[node_index]
        tokens = jnp.take(token_pool[node_index], sample_rows, axis=0)
        cotangent = jnp.take(cotangent_pool[node_index], sample_rows, axis=0)
        gradient = node_gradient(weights[node_index], tokens, cotangent)
        tracked = (residue[node_index].astype(jnp.float32) + gradient).astype(jnp.bfloat16)
        return (tracked, gradient, jnp.sum(gradient * gradient))
    tracked, gradient, squares = lax.map(per_node, jnp.arange(N_NODE, dtype=jnp.int32))
    levels = N_NODE.bit_length() - 1
    offset = jnp.left_shift(jnp.int32(1), round_index[0] % levels)

    def track_node(node_index):
        peer_index = (node_index - offset) % N_NODE
        tracker = 0.5 * (tracked[node_index].astype(jnp.float32) + tracked[peer_index].astype(jnp.float32))
        sent = (weights[node_index].astype(jnp.float32) - step_rate * tracker).astype(jnp.bfloat16)
        return (tracker, sent)
    tracker_all, sent_all = lax.map(track_node, jnp.arange(N_NODE, dtype=jnp.int32))

    def mix_node(node_index):
        peer_index = (node_index - offset) % N_NODE
        tracker = tracker_all[node_index]
        mixed = 0.5 * weights[node_index].astype(jnp.float32) + 0.5 * sent_all[peer_index].astype(jnp.float32) - 0.5 * step_rate * tracker
        return (mixed.astype(jnp.bfloat16), (tracker - gradient[node_index]).astype(jnp.bfloat16))
    new_weights, new_residue = lax.map(mix_node, jnp.arange(N_NODE, dtype=jnp.int32))
    grad_rms = jnp.sqrt(jnp.sum(squares) / (N_NODE * gradient[0].size))
    return (new_weights, new_residue, grad_rms)
```

```python
from functools import partial

import jax
import jax.numpy as jnp
from jax import lax
from jax.experimental import pallas as pl
from jax.experimental.pallas import tpu as pltpu
from jax.sharding import Mesh
from jax.sharding import PartitionSpec as P

NODE = ("z", "x", "y", "core")
SIZES = (8, 4, 4, 2)
HEAD_DIM = 64
step_rate = 0.1

epsilon = 1e-06
bf16, f32 = jnp.bfloat16, jnp.float32


def dot(a, b, ca, cb):
    return lax.dot_general(a, b, (((ca,), (cb,)), ((), ())), preferred_element_type=f32)


def gradient_kernel(ids, tok, cot, w, res, t0, t1, t2, t3, sq, wbuf, rbuf, tbuf, tokb, cotb, proj, grads, sem_in, sem_r, sem_out):
    images, seq, width = tok.shape
    rows = images * seq
    group, head = 256, 64
    outs = (t0, t1, t2, t3)
    scale = width**-0.5
    loads = [pltpu.make_async_copy(tok, tokb, sem_in.at[0]), pltpu.make_async_copy(cot, cotb, sem_in.at[1])]
    wloads = [pltpu.make_async_copy(w.at[m], wbuf.at[m], sem_in.at[2 + m]) for m in range(4)]
    rloads = [pltpu.make_async_copy(res.at[m], rbuf.at[m], sem_r.at[m]) for m in range(4)]
    stores = [pltpu.make_async_copy(tbuf.at[m], outs[m], sem_out.at[m]) for m in range(4)]
    for c in (loads[0], wloads[0], wloads[1], loads[1], wloads[3], wloads[2], *rloads):
        c.start()

    count = [jnp.int32(0)] * images
    for j in range(ids.shape[0]):
        for b in range(images):
            count[b] = count[b] + (ids[j] == b).astype(jnp.int32)
    count = [c.astype(f32) for c in count]

    loads[0].wait()
    values = tokb[...].reshape(rows, width).astype(f32)
    centered = values - jnp.mean(values, -1, keepdims=True)
    variance = jnp.mean(centered * centered, -1, keepdims=True)
    normed = (centered * lax.rsqrt(variance + epsilon)).astype(bf16)
    for m, extra in ((0, head**-0.5), (1, 1.0), (2, 1.0)):
        wloads[m].wait()
        proj[m] = (dot(normed, wbuf[m], 1, 0) * scale).astype(bf16) * bf16(extra)
    loads[1].wait()
    wloads[3].wait()
    grad_rows = cotb[...].reshape(rows, width)
    proj[3] = (dot(grad_rows, wbuf[3], 1, 1) * scale).astype(bf16)

    heads = group // head
    same = (
        lax.broadcasted_iota(jnp.int32, (heads * seq, group), 0) // seq
        == lax.broadcasted_iota(jnp.int32, (heads * seq, group), 1) // head
    )
    own = same.astype(f32).astype(bf16)
    lane_head = lax.broadcasted_iota(jnp.int32, (seq, group), 1) // head

    def diagonal(x):
        out = x[:seq]
        for h in range(1, heads):
            out = jnp.where(lane_head == h, x[h * seq : (h + 1) * seq], out)
        return out

    for b in range(images):
        r = slice(b * seq, (b + 1) * seq)
        for g in range(width // group):
            c = slice(g * group, (g + 1) * group)
            q, k, v, d = (proj[m, r, c] for m in range(4))
            qs = jnp.concatenate([q] * heads, 0) * own
            ds = jnp.concatenate([d] * heads, 0) * own
            s = dot(k, qs, 1, 1)
            e = jnp.exp(s - jnp.max(s, 0, keepdims=True))
            p = e * (1.0 / jnp.sum(e, 0, keepdims=True))
            ph = p.astype(bf16)
            dp = dot(v, ds, 1, 1)
            sg = (p * (dp - jnp.sum(dp * p, 0, keepdims=True)) * count[b]).astype(bf16)
            grads[2, r, c] = (dot(ph, ds, 1, 0) * count[b]).astype(bf16)
            grads[1, r, c] = dot(sg, qs, 1, 0).astype(bf16)
            grads[3, r, c] = (diagonal(dot(ph, v, 0, 0)) * count[b]).astype(bf16)
            grads[0, r, c] = (diagonal(dot(sg, k, 0, 0)) * head**-0.5).astype(bf16)

    total = jnp.zeros((8, width), f32)
    for m in range(4):
        left, right = (grads[3], grad_rows) if m == 3 else (normed, grads[m])
        gradient = dot(left, right, 0, 0) * scale
        rloads[m].wait()
        tbuf[m] = (rbuf[m].astype(f32) + gradient).astype(bf16)
        stores[m].start()
        total = total + jnp.sum((gradient * gradient).reshape(-1, 8, width), 0)
    sq[0] = jnp.sum(total)
    for m in range(4):
        stores[m].wait()


def gradient_call(ids, tok, cot, w, res):
    images, seq, width = tok.shape
    rows = images * seq
    hbm = pl.BlockSpec(memory_space=pl.ANY)
    smem = pl.BlockSpec(memory_space=pltpu.SMEM)
    part = jax.ShapeDtypeStruct((width, width), bf16)
    return pl.pallas_call(
        gradient_kernel,
        in_specs=[smem, hbm, hbm, hbm, hbm],
        out_specs=[hbm] * 4 + [smem],
        out_shape=[part] * 4 + [jax.ShapeDtypeStruct((1,), f32)],
        scratch_shapes=[
            pltpu.VMEM((4, width, width), bf16),
            pltpu.VMEM((4, width, width), bf16),
            pltpu.VMEM((4, width, width), bf16),
            pltpu.VMEM((images, seq, width), bf16),
            pltpu.VMEM((images, seq, width), bf16),
            pltpu.VMEM((4, rows, width), bf16),
            pltpu.VMEM((4, rows, width), bf16),
            pltpu.SemaphoreType.DMA((6,)),
            pltpu.SemaphoreType.DMA((4,)),
            pltpu.SemaphoreType.DMA((4,)),
        ],
        name="gradient",
    )(ids, tok, cot, w, res)


def moved(x, steps):
    total = 256
    route = []
    for i in range(total):
        rest, at = i, []
        for size in reversed(SIZES):
            at.append(rest % size)
            rest //= size
        at = [(a + s) % n for a, s, n in zip(reversed(at), steps, SIZES)]
        j = 0
        for a, n in zip(at, SIZES):
            j = j * n + a
        route.append((i, j))
    return lax.ppermute(x, NODE, route)


def from_behind(x, distance):
    return lax.ppermute(x, NODE, [((i - distance) % 256, i) for i in range(256)])


def sum_over_slice(v):
    for steps in (
        (0, 0, 0, 1),
        (0, 0, 1, 0),
        (0, 0, 2, 0),
        (0, 1, 0, 0),
        (0, 2, 0, 0),
        (1, 0, 0, 0),
        (2, 0, 0, 0),
        (4, 0, 0, 0),
    ):
        v = v + moved(v, steps)
    return v


def tracker_of(own, peer):
    return 0.5 * (own.astype(f32) + peer.astype(f32))


def form_sent(weight, tracker):
    return (weight.astype(f32) - step_rate * tracker).astype(bf16)


def mixed(weight, tracker, peer_sent):
    return (0.5 * weight.astype(f32) + 0.5 * peer_sent.astype(f32) - 0.5 * step_rate * tracker).astype(bf16)


def exchange(distance, weights, residue, squares, *tracked):
    parts = range(len(tracked))
    near = [from_behind(tracked[m], distance) for m in parts]
    total = sum_over_slice(squares)
    trackers = [tracker_of(tracked[m], near[m]) for m in parts]
    sent = [from_behind(form_sent(weights[m], trackers[m]), distance) for m in parts]
    new_weights = jnp.stack([mixed(weights[m], trackers[m], sent[m]) for m in parts])
    new_residue = jnp.stack(
        [(residue[m].astype(f32) + (trackers[m] - tracked[m].astype(f32))).astype(bf16) for m in parts]
    )
    return new_weights, new_residue, total


def exchange_halfway(ids, tok, cot, weights, residue):
    parts = range(weights.shape[0])
    peer_weights = [from_behind(weights[m], 128) for m in parts]
    *tracked, squares = gradient_call(ids, tok, cot, weights, residue)
    near = [from_behind(tracked[m], 128) for m in parts]
    total = sum_over_slice(squares)
    trackers = [tracker_of(tracked[m], near[m]) for m in parts]
    new_weights = jnp.stack([mixed(weights[m], trackers[m], form_sent(peer_weights[m], trackers[m])) for m in parts])
    new_residue = jnp.stack(
        [(residue[m].astype(f32) + (trackers[m] - tracked[m].astype(f32))).astype(bf16) for m in parts]
    )
    return new_weights, new_residue, total


def exchange_any(level, ids, tok, cot, weights, residue):
    *tracked, squares = gradient_call(ids, tok, cot, weights, residue)
    return lax.switch(
        level, [partial(exchange, 2**k) for k in range(7)], weights, residue, squares, *tracked
    )


def per_device(round_index, sample_ids, token_pool, cotangent_pool, weights, residue):
    level = round_index[0] % 8
    args = (sample_ids[0], token_pool[0], cotangent_pool[0], weights[0], residue[0])
    new_weights, new_residue, total = lax.cond(
        level == 7, exchange_halfway, partial(exchange_any, jnp.minimum(level, 6)), *args
    )
    grad_rms = jnp.sqrt(total[0] / (256 * weights[0].size))
    return new_weights[None], new_residue[None], grad_rms


def solution(mesh):
    torus = Mesh(mesh.devices.reshape(SIZES), NODE)
    split = P(NODE, None, None, None)
    return jax.shard_map(
        per_device,
        mesh=torus,
        in_specs=(P(), P(NODE, None), split, split, split, split),
        out_specs=(split, split, P()),
        check_vma=False,
    )
```

```python
from functools import partial

import jax
import jax.numpy as jnp
from jax import lax
from jax.experimental import pallas as pl
from jax.experimental.pallas import tpu as pltpu
from jax.sharding import Mesh
from jax.sharding import PartitionSpec as P

NODE = ("z", "x", "y", "core")
SIZES = (8, 4, 4, 2)
LEVELS = 8
step_rate = 0.1

epsilon = 1e-06
bf16, f32 = jnp.bfloat16, jnp.float32


def dot(a, b, ca, cb):
    return lax.dot_general(a, b, (((ca,), (cb,)), ((), ())), preferred_element_type=f32)


def gradient_kernel(ids, tok, cot, w, res, out, sq, wbuf, rbuf, tbuf, tokb, cotb, proj, grads, sem_in, sem_r, sem_out):
    images, seq, width = tok.shape
    rows = images * seq
    group, head = 256, 64
    scale = width**-0.5
    loads = [pltpu.make_async_copy(tok, tokb, sem_in.at[0]), pltpu.make_async_copy(cot, cotb, sem_in.at[1])]
    wloads = [pltpu.make_async_copy(w.at[m], wbuf.at[m], sem_in.at[2 + m]) for m in range(4)]
    rloads = [pltpu.make_async_copy(res.at[m], rbuf.at[m], sem_r.at[m]) for m in range(4)]
    stores = [pltpu.make_async_copy(tbuf.at[m], out.at[m], sem_out.at[m]) for m in range(4)]
    for c in (loads[0], wloads[0], wloads[1], loads[1], wloads[3], wloads[2], *rloads):
        c.start()

    count = [jnp.int32(0)] * images
    for j in range(ids.shape[0]):
        for b in range(images):
            count[b] = count[b] + (ids[j] == b).astype(jnp.int32)
    count = [c.astype(f32) for c in count]

    loads[0].wait()
    values = tokb[...].reshape(rows, width).astype(f32)
    centered = values - jnp.mean(values, -1, keepdims=True)
    variance = jnp.mean(centered * centered, -1, keepdims=True)
    normed = (centered * lax.rsqrt(variance + epsilon)).astype(bf16)
    for m, extra in ((0, head**-0.5), (1, 1.0), (2, 1.0)):
        wloads[m].wait()
        proj[m] = (dot(normed, wbuf[m], 1, 0) * scale).astype(bf16) * bf16(extra)
    loads[1].wait()
    wloads[3].wait()
    grad_rows = cotb[...].reshape(rows, width)
    proj[3] = (dot(grad_rows, wbuf[3], 1, 1) * scale).astype(bf16)

    heads = group // head
    same = (
        lax.broadcasted_iota(jnp.int32, (heads * seq, group), 0) // seq
        == lax.broadcasted_iota(jnp.int32, (heads * seq, group), 1) // head
    )
    own = same.astype(f32).astype(bf16)
    lane_head = lax.broadcasted_iota(jnp.int32, (seq, group), 1) // head

    def diagonal(x):
        out = x[:seq]
        for h in range(1, heads):
            out = jnp.where(lane_head == h, x[h * seq : (h + 1) * seq], out)
        return out

    for b in range(images):
        r = slice(b * seq, (b + 1) * seq)
        for g in range(width // group):
            c = slice(g * group, (g + 1) * group)
            q, k, v, d = (proj[m, r, c] for m in range(4))
            qs = jnp.concatenate([q] * heads, 0) * own
            ds = jnp.concatenate([d] * heads, 0) * own
            s = dot(k, qs, 1, 1)
            e = jnp.exp(s - jnp.max(s, 0, keepdims=True))
            p = e * (1.0 / jnp.sum(e, 0, keepdims=True))
            ph = p.astype(bf16)
            dp = dot(v, ds, 1, 1)
            sg = (p * (dp - jnp.sum(dp * p, 0, keepdims=True)) * count[b]).astype(bf16)
            grads[2, r, c] = (dot(ph, ds, 1, 0) * count[b]).astype(bf16)
            grads[1, r, c] = dot(sg, qs, 1, 0).astype(bf16)
            grads[3, r, c] = (diagonal(dot(ph, v, 0, 0)) * count[b]).astype(bf16)
            grads[0, r, c] = (diagonal(dot(sg, k, 0, 0)) * head**-0.5).astype(bf16)

    total = jnp.zeros((8, width), f32)
    for m in range(4):
        left, right = (grads[3], grad_rows) if m == 3 else (normed, grads[m])
        gradient = dot(left, right, 0, 0) * scale
        rloads[m].wait()
        tbuf[m] = (rbuf[m].astype(f32) + gradient).astype(bf16)
        stores[m].start()
        total = total + jnp.sum((gradient * gradient).reshape(-1, 8, width), 0)
    sq[0] = jnp.sum(total)
    for m in range(4):
        stores[m].wait()


def gradient_call(ids, tok, cot, w, res):
    images, seq, width = tok.shape
    rows = images * seq
    hbm = pl.BlockSpec(memory_space=pl.ANY)
    smem = pl.BlockSpec(memory_space=pltpu.SMEM)
    return pl.pallas_call(
        gradient_kernel,
        in_specs=[smem, hbm, hbm, hbm, hbm],
        out_specs=[hbm, smem],
        out_shape=[jax.ShapeDtypeStruct(w.shape, bf16), jax.ShapeDtypeStruct((1,), f32)],
        scratch_shapes=[
            pltpu.VMEM((4, width, width), bf16),
            pltpu.VMEM((4, width, width), bf16),
            pltpu.VMEM((4, width, width), bf16),
            pltpu.VMEM((images, seq, width), bf16),
            pltpu.VMEM((images, seq, width), bf16),
            pltpu.VMEM((4, rows, width), bf16),
            pltpu.VMEM((4, rows, width), bf16),
            pltpu.SemaphoreType.DMA((6,)),
            pltpu.SemaphoreType.DMA((4,)),
            pltpu.SemaphoreType.DMA((4,)),
        ],
        name="gradient",
    )(ids, tok, cot, w, res)


def from_behind(x, distance):
    return lax.ppermute(x, NODE, [((i - distance) % 256, i) for i in range(256)])


def sum_over(v, axes):
    for axis in axes:
        v = lax.psum(v, axis)
    return v


def busy_axis(level):
    return "y" if level < 3 else "x" if level < 5 else "z"


def tracker_of(own, peer):
    return 0.5 * (own.astype(f32) + peer.astype(f32))


def form_sent(weights, tracker):
    return (weights.astype(f32) - step_rate * tracker).astype(bf16)


def mixed(weights, tracker, peer_sent):
    return (0.5 * weights.astype(f32) + 0.5 * peer_sent.astype(f32) - 0.5 * step_rate * tracker).astype(bf16)


def kept(residue, tracked, tracker):
    return (residue.astype(f32) + (tracker - tracked.astype(f32))).astype(bf16)


def bring_tracked(level, tracked, squares):
    near = from_behind(tracked, 2**level)
    return near, sum_over(squares, [a for a in NODE if a != busy_axis(level)])


def bring_sent(level, own_sent, total):
    return from_behind(own_sent, 2**level), lax.psum(total, busy_axis(level))


def per_device(round_index, sample_ids, token_pool, cotangent_pool, weights, residue):
    level = round_index[0] % LEVELS
    weights, residue = weights[0], residue[0]
    tracked, squares = gradient_call(sample_ids[0], token_pool[0], cotangent_pool[0], weights, residue)
    near, total = lax.switch(level, [partial(bring_tracked, k) for k in range(LEVELS)], tracked, squares)
    tracker = tracker_of(tracked, near)
    sent, total = lax.switch(
        level, [partial(bring_sent, k) for k in range(LEVELS)], form_sent(weights, tracker), total
    )
    grad_rms = jnp.sqrt(total[0] / (256 * weights.size))
    return mixed(weights, tracker, sent)[None], kept(residue, tracked, tracker)[None], grad_rms


def solution(mesh):
    torus = Mesh(mesh.devices.reshape(SIZES), NODE)
    split = P(NODE, None, None, None)
    return jax.shard_map(
        per_device,
        mesh=torus,
        in_specs=(P(), P(NODE, None), split, split, split, split),
        out_specs=(split, split, P()),
        check_vma=False,
    )
```

```python
from functools import partial

import jax
import jax.numpy as jnp
from jax import lax
from jax.experimental import pallas as pl
from jax.experimental.pallas import tpu as pltpu
from jax.sharding import Mesh
from jax.sharding import PartitionSpec as P

NODE = ("z", "x", "y", "core")
SIZES = (8, 4, 4, 2)
LEVELS = 8
CUT = 1568
step_rate = 0.1

epsilon = 1e-06
PARTS = (2048,)
bf16, f32 = jnp.bfloat16, jnp.float32


def dot(a, b, ca, cb):
    return lax.dot_general(a, b, (((ca,), (cb,)), ((), ())), preferred_element_type=f32)


def gradient_kernel(ids, tok, cot, w, res, out0, sq, wbuf, rbuf, tbuf, tokb, cotb, proj, grads, sem_in, sem_r, sem_out):
    images, seq, width = tok.shape
    rows = images * seq
    group, head = 256, 64
    outs = (out0,)
    scale = width**-0.5
    loads = [pltpu.make_async_copy(tok, tokb, sem_in.at[0]), pltpu.make_async_copy(cot, cotb, sem_in.at[1])]
    wloads = [pltpu.make_async_copy(w.at[m], wbuf.at[m], sem_in.at[2 + m]) for m in range(4)]
    rloads = [pltpu.make_async_copy(res.at[m], rbuf.at[m], sem_r.at[m]) for m in range(4)]
    pieces, row = [], 0
    for out in outs:
        start, end = row, row + out.shape[0]
        while row < end:
            m, at = divmod(row, width)
            size = min(end - row, width - at)
            pieces.append((pl.ds(at, size), out.at[pl.ds(row - start, size)], m))
            row += size
    stores = [pltpu.make_async_copy(tbuf.at[m, r], o, sem_out.at[j]) for j, (r, o, m) in enumerate(pieces)]
    for c in (loads[0], wloads[0], wloads[1], loads[1], wloads[3], wloads[2], *rloads):
        c.start()

    count = [jnp.int32(0)] * images
    for j in range(ids.shape[0]):
        for b in range(images):
            count[b] = count[b] + (ids[j] == b).astype(jnp.int32)
    count = [c.astype(f32) for c in count]

    loads[0].wait()
    values = tokb[...].reshape(rows, width).astype(f32)
    centered = values - jnp.mean(values, -1, keepdims=True)
    variance = jnp.mean(centered * centered, -1, keepdims=True)
    normed = (centered * lax.rsqrt(variance + epsilon)).astype(bf16)
    for m, extra in ((0, head**-0.5), (1, 1.0), (2, 1.0)):
        wloads[m].wait()
        proj[m] = (dot(normed, wbuf[m], 1, 0) * scale).astype(bf16) * bf16(extra)
    loads[1].wait()
    wloads[3].wait()
    grad_rows = cotb[...].reshape(rows, width)
    proj[3] = (dot(grad_rows, wbuf[3], 1, 1) * scale).astype(bf16)

    heads = group // head
    same = (
        lax.broadcasted_iota(jnp.int32, (heads * seq, group), 0) // seq
        == lax.broadcasted_iota(jnp.int32, (heads * seq, group), 1) // head
    )
    own = same.astype(f32).astype(bf16)
    lane_head = lax.broadcasted_iota(jnp.int32, (seq, group), 1) // head

    def diagonal(x):
        out = x[:seq]
        for h in range(1, heads):
            out = jnp.where(lane_head == h, x[h * seq : (h + 1) * seq], out)
        return out

    for b in range(images):
        r = slice(b * seq, (b + 1) * seq)
        for g in range(width // group):
            c = slice(g * group, (g + 1) * group)
            q, k, v, d = (proj[m, r, c] for m in range(4))
            qs = jnp.concatenate([q] * heads, 0) * own
            ds = jnp.concatenate([d] * heads, 0) * own
            s = dot(k, qs, 1, 1)
            e = jnp.exp(s - jnp.max(s, 0, keepdims=True))
            p = e * (1.0 / jnp.sum(e, 0, keepdims=True))
            ph = p.astype(bf16)
            dp = dot(v, ds, 1, 1)
            sg = (p * (dp - jnp.sum(dp * p, 0, keepdims=True)) * count[b]).astype(bf16)
            grads[2, r, c] = (dot(ph, ds, 1, 0) * count[b]).astype(bf16)
            grads[1, r, c] = dot(sg, qs, 1, 0).astype(bf16)
            grads[3, r, c] = (diagonal(dot(ph, v, 0, 0)) * count[b]).astype(bf16)
            grads[0, r, c] = (diagonal(dot(sg, k, 0, 0)) * head**-0.5).astype(bf16)

    total = jnp.zeros((8, width), f32)
    for m in range(4):
        left, right = (grads[3], grad_rows) if m == 3 else (normed, grads[m])
        gradient = dot(left, right, 0, 0) * scale
        rloads[m].wait()
        tbuf[m] = (rbuf[m].astype(f32) + gradient).astype(bf16)
        for store, piece in zip(stores, pieces):
            if piece[2] == m:
                store.start()
        total = total + jnp.sum((gradient * gradient).reshape(-1, 8, width), 0)
    sq[0] = jnp.sum(total)
    for store in stores:
        store.wait()


def gradient_call(ids, tok, cot, w, res):
    images, seq, width = tok.shape
    rows = images * seq
    hbm = pl.BlockSpec(memory_space=pl.ANY)
    smem = pl.BlockSpec(memory_space=pltpu.SMEM)
    return pl.pallas_call(
        gradient_kernel,
        in_specs=[smem, hbm, hbm, hbm, hbm],
        out_specs=[hbm, smem],
        out_shape=[jax.ShapeDtypeStruct((n, width), bf16) for n in PARTS] + [jax.ShapeDtypeStruct((1,), f32)],
        scratch_shapes=[
            pltpu.VMEM((4, width, width), bf16),
            pltpu.VMEM((4, width, width), bf16),
            pltpu.VMEM((4, width, width), bf16),
            pltpu.VMEM((images, seq, width), bf16),
            pltpu.VMEM((images, seq, width), bf16),
            pltpu.VMEM((4, rows, width), bf16),
            pltpu.VMEM((4, rows, width), bf16),
            pltpu.SemaphoreType.DMA((6,)),
            pltpu.SemaphoreType.DMA((4,)),
            pltpu.SemaphoreType.DMA((4,)),
        ],
        name="gradient",
    )(ids, tok, cot, w, res)


def streamed(formula, sources, count, block=256):
    rows, width = sources[0].shape
    steps = rows // block
    total = len(sources) + count

    def kernel(*refs):
        hbm, vmem, sems = refs[:total], refs[total : 2 * total], refs[2 * total]

        def copy(j, i):
            here = pl.ds(i * block, block)
            ends = (hbm[j].at[here], vmem[j].at[here])
            return pltpu.make_async_copy(*(ends if j < len(sources) else ends[::-1]), sems.at[j, i])

        for i in range(steps):
            for j in range(len(sources)):
                copy(j, i).start()

        @pl.loop(0, steps)
        def _(i):
            for j in range(len(sources)):
                copy(j, i).wait()
            here = pl.ds(i * block, block)
            for j, part in enumerate(formula(*(v[here] for v in vmem[: len(sources)]))):
                vmem[len(sources) + j][here] = part
                copy(len(sources) + j, i).start()

        @pl.loop(0, steps)
        def _(i):
            for j in range(len(sources), total):
                copy(j, i).wait()

    return pl.pallas_call(
        kernel,
        in_specs=[pl.BlockSpec(memory_space=pl.ANY)] * len(sources),
        out_specs=[pl.BlockSpec(memory_space=pl.ANY)] * count,
        out_shape=[jax.ShapeDtypeStruct((rows, width), bf16)] * count,
        scratch_shapes=[pltpu.VMEM((rows, width), bf16)] * total + [pltpu.SemaphoreType.DMA((total, steps))],
        name="streamed",
    )(*sources)


def coordinates(i):
    at = []
    for size in reversed(SIZES):
        at.append(i % size)
        i //= size
    return at[::-1]


def node_at(at):
    i = 0
    for a, size in zip(at, SIZES):
        i = i * size + a % size
    return i


def shifted(i, axis, steps):
    at = coordinates(i)
    at[NODE.index(axis)] += steps
    return node_at(at)


def routed(x, target, halves=False):
    pairs = [(i, target(i)) for i in range(256)]
    if halves:
        return sum(lax.ppermute(x, NODE, [p for p in pairs if p[1] % 2 == core]) for core in (0, 1))
    return lax.ppermute(x, NODE, pairs)


def chain_sum(v, axis, halves):
    def down(v, steps):
        return routed(v, lambda i: shifted(i, axis, -steps), halves)

    v = v + down(v, 1)
    if SIZES[NODE.index(axis)] == 4:
        return v + down(down(v, 1), 1)
    v = v + down(v, 2)
    return v + down(down(v, 2), 2)


def sum_over(v, axes):
    for axis in axes:
        v = lax.psum(v, axis)
    return v


def after_tracked(tracked, near, weights, residue):
    tracked, near = tracked.astype(f32), near.astype(f32)
    sent = weights.astype(f32) - step_rate * (0.5 * (tracked + near))
    return sent.astype(bf16), (residue.astype(f32) + 0.5 * (near - tracked)).astype(bf16)


def after_sent(own_sent, sent):
    return ((0.5 * (own_sent.astype(f32) + sent.astype(f32))).astype(bf16),)


def first_sum(level, v):
    if level > 4:
        return sum_over(v, ("y", "x", "core"))
    if level > 2:
        return chain_sum(sum_over(v, ("y", "core")), "z", True)
    return lax.psum(v, "core")


def second_sum(level, v):
    if level > 4:
        return lax.psum(v, "z")
    if level > 2:
        return lax.psum(v, "x")
    if level > 0:
        return sum_over(chain_sum(v, "z", True), ("y", "x"))
    return sum_over(v, ("y", "x", "z"))


def bring(level, x):
    ahead = lambda i: (i + 2**level) % 256
    if level != 6:
        return routed(x, ahead)
    with jax.named_scope("long"):
        hop = routed(x[CUT:], lambda i: shifted(i, "z", -3))
    with jax.named_scope("short"):
        near = routed(x[:CUT], ahead)
    return jnp.concatenate([near, routed(hop, lambda i: shifted(i, "z", -3))])


def bring_tracked(level, tracked, squares):
    return bring(level, tracked), first_sum(level, squares)


def bring_sent(level, own_sent, total):
    return bring(level, own_sent), second_sum(level, total)


def per_device(round_index, sample_ids, token_pool, cotangent_pool, weights, residue):
    level = round_index[0] % LEVELS
    shape = weights.shape
    tracked, squares = gradient_call(sample_ids[0], token_pool[0], cotangent_pool[0], weights[0], residue[0])
    near, total = lax.switch(level, [partial(bring_tracked, k) for k in range(LEVELS)], tracked, squares)
    weights, residue = weights.reshape(-1, shape[-1]), residue.reshape(-1, shape[-1])
    own_sent, new_residue = streamed(after_tracked, (tracked, near, weights, residue), 2)
    sent, total = lax.switch(level, [partial(bring_sent, k) for k in range(LEVELS)], own_sent, total)
    grad_rms = jnp.sqrt(total[0] / (256 * weights.size))
    (new_weights,) = streamed(after_sent, (own_sent, sent), 1)
    return new_weights.reshape(shape), new_residue.reshape(shape), grad_rms


def solution(mesh):
    torus = Mesh(mesh.devices.reshape(SIZES), NODE)
    split = P(NODE, None, None, None)
    return jax.shard_map(
        per_device,
        mesh=torus,
        in_specs=(P(), P(NODE, None), split, split, split, split),
        out_specs=(split, split, P()),
        check_vma=False,
    )
```

```python
from functools import partial

import jax
import jax.numpy as jnp
from jax import lax
from jax.experimental import pallas as pl
from jax.experimental.pallas import tpu as pltpu
from jax.sharding import Mesh
from jax.sharding import PartitionSpec as P

NODE = ("z", "x", "y", "core")
SIZES = (8, 4, 4, 2)
LEVELS = 8
CUT = 1568
step_rate = 0.1

epsilon = 1e-06
PARTS = (2048,)
bf16, f32 = jnp.bfloat16, jnp.float32


def dot(a, b, ca, cb):
    return lax.dot_general(a, b, (((ca,), (cb,)), ((), ())), preferred_element_type=f32)


def gradient_kernel(looped, ids, tok, cot, w, res, out0, sq, wbuf, rbuf, tbuf, tokb, cotb, proj, grads, sem_in, sem_r, sem_out):
    images, seq, width = tok.shape
    rows = images * seq
    group, head = 256, 64
    outs = (out0,)
    scale = width**-0.5
    loads = [pltpu.make_async_copy(tok, tokb, sem_in.at[0]), pltpu.make_async_copy(cot, cotb, sem_in.at[1])]
    wloads = [pltpu.make_async_copy(w.at[m], wbuf.at[m], sem_in.at[2 + m]) for m in range(4)]
    rloads = [pltpu.make_async_copy(res.at[m], rbuf.at[m], sem_r.at[m]) for m in range(4)]
    pieces, row = [], 0
    for out in outs:
        start, end = row, row + out.shape[0]
        while row < end:
            m, at = divmod(row, width)
            size = min(end - row, width - at)
            pieces.append((pl.ds(at, size), out.at[pl.ds(row - start, size)], m))
            row += size
    stores = [pltpu.make_async_copy(tbuf.at[m, r], o, sem_out.at[j]) for j, (r, o, m) in enumerate(pieces)]
    for c in (loads[0], wloads[0], wloads[1], loads[1], wloads[3], wloads[2], *rloads):
        c.start()

    count = [jnp.int32(0)] * images
    for j in range(ids.shape[0]):
        for b in range(images):
            count[b] = count[b] + (ids[j] == b).astype(jnp.int32)
    count = [c.astype(f32) for c in count]

    loads[0].wait()
    values = tokb[...].reshape(rows, width).astype(f32)
    centered = values - jnp.mean(values, -1, keepdims=True)
    variance = jnp.mean(centered * centered, -1, keepdims=True)
    normed = (centered * lax.rsqrt(variance + epsilon)).astype(bf16)
    for m, extra in ((0, head**-0.5), (1, 1.0), (2, 1.0)):
        wloads[m].wait()
        proj[m] = (dot(normed, wbuf[m], 1, 0) * scale).astype(bf16) * bf16(extra)
    loads[1].wait()
    wloads[3].wait()
    grad_rows = cotb[...].reshape(rows, width)
    proj[3] = (dot(grad_rows, wbuf[3], 1, 1) * scale).astype(bf16)

    heads = group // head
    same = (
        lax.broadcasted_iota(jnp.int32, (heads * seq, group), 0) // seq
        == lax.broadcasted_iota(jnp.int32, (heads * seq, group), 1) // head
    )
    own = same.astype(f32).astype(bf16)
    lane_head = lax.broadcasted_iota(jnp.int32, (seq, group), 1) // head

    def diagonal(x):
        out = x[:seq]
        for h in range(1, heads):
            out = jnp.where(lane_head == h, x[h * seq : (h + 1) * seq], out)
        return out

    def attend(b, share):
        r = pl.ds(b * seq if isinstance(b, int) else pl.multiple_of(b * seq, seq), seq)
        for g in range(width // group):
            c = slice(g * group, (g + 1) * group)
            q, k, v, d = (proj[m, r, c] for m in range(4))
            qs = jnp.concatenate([q] * heads, 0) * own
            ds = jnp.concatenate([d] * heads, 0) * own
            s = dot(k, qs, 1, 1)
            e = jnp.exp(s - jnp.max(s, 0, keepdims=True))
            p = e * (1.0 / jnp.sum(e, 0, keepdims=True))
            ph = p.astype(bf16)
            dp = dot(v, ds, 1, 1)
            sg = (p * (dp - jnp.sum(dp * p, 0, keepdims=True)) * share).astype(bf16)
            grads[2, r, c] = (dot(ph, ds, 1, 0) * share).astype(bf16)
            grads[1, r, c] = dot(sg, qs, 1, 0).astype(bf16)
            grads[3, r, c] = (diagonal(dot(ph, v, 0, 0)) * share).astype(bf16)
            grads[0, r, c] = (diagonal(dot(sg, k, 0, 0)) * head**-0.5).astype(bf16)

    if looped:

        @pl.loop(0, images)
        def _(b):
            share = jnp.int32(0)
            for j in range(ids.shape[0]):
                share = share + (ids[j] == b).astype(jnp.int32)
            attend(b, share.astype(f32))

    else:
        for b in range(images):
            attend(b, count[b])

    total = jnp.zeros((8, width), f32)
    for m in range(4):
        left, right = (grads[3], grad_rows) if m == 3 else (normed, grads[m])
        gradient = dot(left, right, 0, 0) * scale
        rloads[m].wait()
        tbuf[m] = (rbuf[m].astype(f32) + gradient).astype(bf16)
        for store, piece in zip(stores, pieces):
            if piece[2] == m:
                store.start()
        total = total + jnp.sum((gradient * gradient).reshape(-1, 8, width), 0)
    sq[0] = jnp.sum(total)
    for store in stores:
        store.wait()


def gradient_call(ids, tok, cot, w, res, looped=False):
    images, seq, width = tok.shape
    rows = images * seq
    hbm = pl.BlockSpec(memory_space=pl.ANY)
    smem = pl.BlockSpec(memory_space=pltpu.SMEM)
    return pl.pallas_call(
        partial(gradient_kernel, looped),
        in_specs=[smem, hbm, hbm, hbm, hbm],
        out_specs=[hbm, smem],
        out_shape=[jax.ShapeDtypeStruct((n, width), bf16) for n in PARTS] + [jax.ShapeDtypeStruct((1,), f32)],
        scratch_shapes=[
            pltpu.VMEM((4, width, width), bf16),
            pltpu.VMEM((4, width, width), bf16),
            pltpu.VMEM((4, width, width), bf16),
            pltpu.VMEM((images, seq, width), bf16),
            pltpu.VMEM((images, seq, width), bf16),
            pltpu.VMEM((4, rows, width), bf16),
            pltpu.VMEM((4, rows, width), bf16),
            pltpu.SemaphoreType.DMA((6,)),
            pltpu.SemaphoreType.DMA((4,)),
            pltpu.SemaphoreType.DMA((4,)),
        ],
        name="gradient",
    )(ids, tok, cot, w, res)


def streamed(formula, sources, count, block=256):
    rows, width = sources[0].shape
    steps, inputs, total = rows // block, len(sources), len(sources) + count

    def kernel(*refs):
        hbm, vmem, sems = refs[:total], refs[total : 2 * total], refs[2 * total]

        def copy(j, i):
            here = pl.ds(i * block, block)
            ends = (hbm[j].at[here], vmem[j].at[here])
            return pltpu.make_async_copy(*(ends if j < inputs else ends[::-1]), sems.at[j, i])

        @pl.loop(0, steps)
        def _(i):
            for j in range(inputs):
                copy(j, i).start()

        @pl.loop(0, steps)
        def _(i):
            for j in range(inputs):
                copy(j, i).wait()

            @pl.loop(0, block // 32)
            def _(k):
                here = pl.ds(pl.multiple_of(i * block + k * 32, 32), 32)
                for j, part in enumerate(formula(*(v[here] for v in vmem[:inputs]))):
                    vmem[inputs + j][here] = part

            for j in range(inputs, total):
                copy(j, i).start()

        @pl.loop(0, steps)
        def _(i):
            for j in range(inputs, total):
                copy(j, i).wait()

    return pl.pallas_call(
        kernel,
        in_specs=[pl.BlockSpec(memory_space=pl.ANY)] * inputs,
        out_specs=[pl.BlockSpec(memory_space=pl.ANY)] * count,
        out_shape=[jax.ShapeDtypeStruct((rows, width), bf16)] * count,
        scratch_shapes=[pltpu.VMEM((rows, width), bf16)] * total + [pltpu.SemaphoreType.DMA((total, steps))],
        name="streamed",
    )(*sources)


def copied(sources, sizes):
    width, rows = sources[0].shape[1], sum(sizes)

    def places(heights):
        return [(side, row) for side, n in enumerate(heights) for row in range(n)]

    begin, end = places([s.shape[0] for s in sources]), places(sizes)
    cuts = sorted({0, rows, *range(0, rows, 512)} | {r for r in range(rows) if 0 in (begin[r][1], end[r][1])})
    moves = [(begin[r], end[r], r, n - r) for r, n in zip(cuts, cuts[1:])]

    def kernel(*refs):
        inputs, outs, (held, loaded, stored) = refs[: len(sources)], refs[len(sources) : -3], refs[-3:]
        loads, stores = [], []
        for j, ((s, i), (d, o), r, n) in enumerate(moves):
            here = held.at[pl.ds(r, n)]
            loads.append(pltpu.make_async_copy(inputs[s].at[pl.ds(i, n)], here, loaded.at[j]))
            stores.append(pltpu.make_async_copy(here, outs[d].at[pl.ds(o, n)], stored.at[j]))
        for load in loads:
            load.start()
        for load, store in zip(loads, stores):
            load.wait()
            store.start()
        for store in stores:
            store.wait()

    return pl.pallas_call(
        kernel,
        in_specs=[pl.BlockSpec(memory_space=pl.ANY)] * len(sources),
        out_specs=[pl.BlockSpec(memory_space=pl.ANY)] * len(sizes),
        out_shape=[jax.ShapeDtypeStruct((n, width), bf16) for n in sizes],
        scratch_shapes=[pltpu.VMEM((rows, width), bf16)] + [pltpu.SemaphoreType.DMA((len(moves),))] * 2,
        name="copied",
    )(*sources)


def coordinates(i):
    at = []
    for size in reversed(SIZES):
        at.append(i % size)
        i //= size
    return at[::-1]


def node_at(at):
    i = 0
    for a, size in zip(at, SIZES):
        i = i * size + a % size
    return i


def shifted(i, axis, steps):
    at = coordinates(i)
    at[NODE.index(axis)] += steps
    return node_at(at)


def routed(x, target):
    return lax.ppermute(x, NODE, [(i, target(i)) for i in range(256)])


def ring_sum(v, axis):
    def step(_, carry):
        moving, total = carry
        moving = routed(moving, lambda i: shifted(i, axis, -1))
        return moving, total + moving

    return lax.fori_loop(1, SIZES[NODE.index(axis)], step, (v, v))[1]


def sum_over(v, axes):
    for axis in axes:
        v = lax.psum(v, axis)
    return v


def form_sent(tracked, near, weights):
    tracker = 0.5 * (tracked.astype(f32) + near.astype(f32))
    return ((weights.astype(f32) - step_rate * tracker).astype(bf16),)


def kept(tracked, near, residue):
    return ((residue.astype(f32) + 0.5 * (near.astype(f32) - tracked.astype(f32))).astype(bf16),)


def mixed(own_sent, sent):
    return ((0.5 * (own_sent.astype(f32) + sent.astype(f32))).astype(bf16),)


def both(tracked, near, weights, peer_weights, residue):
    (own_sent,), (sent,) = form_sent(tracked, near, weights), form_sent(near, tracked, peer_weights)
    return *mixed(own_sent, sent), *kept(tracked, near, residue)


def first_sum(level, v):
    if level > 5:
        return sum_over(v, ("y", "x", "core"))
    return ring_sum(v, "z") if level > 0 else lax.psum(v, "core")


def second_sum(level, v):
    if level > 5:
        return lax.psum(v, "z")
    if level > 2:
        return sum_over(v, ("y", "core", "x"))
    return sum_over(ring_sum(v, "x"), ("core", "y")) if level > 0 else sum_over(v, ("y", "x", "z"))


def flat(x):
    return x.reshape(-1, x.shape[-1])


def after(x, *others):
    return lax.optimization_barrier((x, *others))[0]


def bring(level, x):
    ahead = lambda i: (i + 2**level) % 256
    if level != 6:
        return routed(x, ahead), lambda v: v
    large, small = copied([x], (CUT, x.shape[0] - CUT))
    three_down = lambda i: shifted(i, "z", -3)
    hop = routed(small, three_down)
    near = routed(large, ahead)
    return (near, hop), lambda pair, v: copied([pair[0], routed(after(pair[1], v), three_down)], (x.shape[0],))[0]


def bring_tracked(level, tracked, squares):
    near, finish = bring(level, tracked)
    total = first_sum(level, squares)
    return (finish(near, total) if level == 6 else near), total


def bring_sent(level, own_sent, total, tracked, near, residue):
    sent, finish = bring(level, own_sent)
    (new_residue,) = streamed(kept, (tracked, near, residue), 1)
    if level == 6:
        sent = finish(sent, new_residue)
    total = second_sum(level, after(total, new_residue))
    return sent, new_residue, total


def round_of(level, ids, tok, cot, weights, residue):
    tracked, squares = gradient_call(ids, tok, cot, weights, residue)
    branches = range(LEVELS - 1)
    near, total = lax.switch(level, [partial(bring_tracked, k) for k in branches], tracked, squares)
    (own_sent,) = streamed(form_sent, (tracked, near, flat(weights)), 1)
    sent, new_residue, total = lax.switch(
        level, [partial(bring_sent, k) for k in branches], own_sent, total, tracked, near, flat(residue)
    )
    (new_weights,) = streamed(mixed, (own_sent, sent), 1)
    return new_weights, new_residue, total


def halfway_round(ids, tok, cot, weights, residue):
    ahead = lambda i: (i + 128) % 256
    peer_weights = routed(flat(weights), ahead)
    tracked, squares = gradient_call(ids, tok, cot, weights, residue, looped=True)
    near = routed(tracked, ahead)
    total = sum_over(squares, ("y", "x", "core", "z"))
    new_weights, new_residue = streamed(both, (tracked, near, flat(weights), peer_weights, flat(residue)), 2)
    return new_weights, new_residue, total


def per_device(round_index, sample_ids, token_pool, cotangent_pool, weights, residue):
    level = round_index[0] % LEVELS
    new_weights, new_residue, total = lax.cond(
        level == LEVELS - 1,
        halfway_round,
        partial(round_of, jnp.minimum(level, LEVELS - 2)),
        sample_ids[0],
        token_pool[0],
        cotangent_pool[0],
        weights[0],
        residue[0],
    )
    grad_rms = jnp.sqrt(total.reshape(()) / (256 * weights.size))
    return new_weights.reshape(weights.shape), new_residue.reshape(weights.shape), grad_rms


def solution(mesh):
    torus = Mesh(mesh.devices.reshape(SIZES), NODE)
    split = P(NODE, None, None, None)
    return jax.shard_map(
        per_device,
        mesh=torus,
        in_specs=(P(), P(NODE, None), split, split, split, split),
        out_specs=(split, split, P()),
        check_vma=False,
    )
```

```python
from functools import partial

import jax
import jax.numpy as jnp
from jax import lax
from jax.experimental import pallas as pl
from jax.experimental.pallas import tpu as pltpu
from jax.sharding import Mesh
from jax.sharding import PartitionSpec as P

NODE = ("z", "x", "y", "core")
SIZES = (8, 4, 4, 2)
LEVELS = 8
CUT = 1568
step_rate = 0.1

epsilon = 1e-06
PARTS = (2048,)
bf16, f32 = jnp.bfloat16, jnp.float32


def dot(a, b, ca, cb):
    return lax.dot_general(a, b, (((ca,), (cb,)), ((), ())), preferred_element_type=f32)


def gradient_kernel(looped, ids, tok, cot, w, res, out0, sq, wbuf, rbuf, tbuf, tokb, cotb, proj, grads, sem_in, sem_r, sem_out):
    images, seq, width = tok.shape
    rows = images * seq
    group, head = 256, 64
    outs = (out0,)
    scale = width**-0.5
    loads = [pltpu.make_async_copy(tok, tokb, sem_in.at[0]), pltpu.make_async_copy(cot, cotb, sem_in.at[1])]
    wloads = [pltpu.make_async_copy(w.at[m], wbuf.at[m], sem_in.at[2 + m]) for m in range(4)]
    rloads = [pltpu.make_async_copy(res.at[m], rbuf.at[m], sem_r.at[m]) for m in range(4)]
    pieces, row = [], 0
    for out in outs:
        start, end = row, row + out.shape[0]
        while row < end:
            m, at = divmod(row, width)
            size = min(end - row, width - at)
            pieces.append((pl.ds(at, size), out.at[pl.ds(row - start, size)], m))
            row += size
    stores = [pltpu.make_async_copy(tbuf.at[m, r], o, sem_out.at[j]) for j, (r, o, m) in enumerate(pieces)]
    for c in (loads[0], wloads[0], wloads[1], loads[1], wloads[3], wloads[2], *rloads):
        c.start()

    count = [jnp.int32(0)] * images
    for j in range(ids.shape[0]):
        for b in range(images):
            count[b] = count[b] + (ids[j] == b).astype(jnp.int32)
    count = [c.astype(f32) for c in count]

    loads[0].wait()
    values = tokb[...].reshape(rows, width).astype(f32)
    centered = values - jnp.mean(values, -1, keepdims=True)
    variance = jnp.mean(centered * centered, -1, keepdims=True)
    normed = (centered * lax.rsqrt(variance + epsilon)).astype(bf16)
    for m, extra in ((0, head**-0.5), (1, 1.0), (2, 1.0)):
        wloads[m].wait()
        proj[m] = (dot(normed, wbuf[m], 1, 0) * scale).astype(bf16) * bf16(extra)
    loads[1].wait()
    wloads[3].wait()
    grad_rows = cotb[...].reshape(rows, width)
    proj[3] = (dot(grad_rows, wbuf[3], 1, 1) * scale).astype(bf16)

    heads = group // head
    same = (
        lax.broadcasted_iota(jnp.int32, (heads * seq, group), 0) // seq
        == lax.broadcasted_iota(jnp.int32, (heads * seq, group), 1) // head
    )
    own = same.astype(f32).astype(bf16)
    lane_head = lax.broadcasted_iota(jnp.int32, (seq, group), 1) // head

    def diagonal(x):
        out = x[:seq]
        for h in range(1, heads):
            out = jnp.where(lane_head == h, x[h * seq : (h + 1) * seq], out)
        return out

    def attend(b, share):
        r = pl.ds(b * seq if isinstance(b, int) else pl.multiple_of(b * seq, seq), seq)
        for g in range(width // group):
            c = slice(g * group, (g + 1) * group)
            q, k, v, d = (proj[m, r, c] for m in range(4))
            qs = jnp.concatenate([q] * heads, 0) * own
            ds = jnp.concatenate([d] * heads, 0) * own
            s = dot(k, qs, 1, 1)
            e = jnp.exp(s - jnp.max(s, 0, keepdims=True))
            p = e * (1.0 / jnp.sum(e, 0, keepdims=True))
            ph = p.astype(bf16)
            dp = dot(v, ds, 1, 1)
            sg = (p * (dp - jnp.sum(dp * p, 0, keepdims=True)) * share).astype(bf16)
            grads[2, r, c] = (dot(ph, ds, 1, 0) * share).astype(bf16)
            grads[1, r, c] = dot(sg, qs, 1, 0).astype(bf16)
            grads[3, r, c] = (diagonal(dot(ph, v, 0, 0)) * share).astype(bf16)
            grads[0, r, c] = (diagonal(dot(sg, k, 0, 0)) * head**-0.5).astype(bf16)

    if looped:

        @pl.loop(0, images)
        def _(b):
            share = jnp.int32(0)
            for j in range(ids.shape[0]):
                share = share + (ids[j] == b).astype(jnp.int32)
            attend(b, share.astype(f32))

    else:
        for b in range(images):
            attend(b, count[b])

    total = jnp.zeros((8, width), f32)
    for m in range(4):
        left, right = (grads[3], grad_rows) if m == 3 else (normed, grads[m])
        gradient = dot(left, right, 0, 0) * scale
        rloads[m].wait()
        tbuf[m] = (rbuf[m].astype(f32) + gradient).astype(bf16)
        for store, piece in zip(stores, pieces):
            if piece[2] == m:
                store.start()
        total = total + jnp.sum((gradient * gradient).reshape(-1, 8, width), 0)
    sq[0] = jnp.sum(total)
    for store in stores:
        store.wait()


def gradient_call(ids, tok, cot, w, res, looped=False):
    images, seq, width = tok.shape
    rows = images * seq
    hbm = pl.BlockSpec(memory_space=pl.ANY)
    smem = pl.BlockSpec(memory_space=pltpu.SMEM)
    return pl.pallas_call(
        partial(gradient_kernel, looped),
        in_specs=[smem, hbm, hbm, hbm, hbm],
        out_specs=[hbm, smem],
        out_shape=[jax.ShapeDtypeStruct((n, width), bf16) for n in PARTS] + [jax.ShapeDtypeStruct((1,), f32)],
        scratch_shapes=[
            pltpu.VMEM((4, width, width), bf16),
            pltpu.VMEM((4, width, width), bf16),
            pltpu.VMEM((4, width, width), bf16),
            pltpu.VMEM((images, seq, width), bf16),
            pltpu.VMEM((images, seq, width), bf16),
            pltpu.VMEM((4, rows, width), bf16),
            pltpu.VMEM((4, rows, width), bf16),
            pltpu.SemaphoreType.DMA((6,)),
            pltpu.SemaphoreType.DMA((4,)),
            pltpu.SemaphoreType.DMA((4,)),
        ],
        name="gradient",
    )(ids, tok, cot, w, res)


def streamed(formula, sources, count, unit=128, block=256):
    rows, width = sources[0].shape
    steps, inputs, total = rows // block, len(sources), len(sources) + count

    def kernel(*refs):
        hbm, vmem, sems = refs[:total], refs[total : 2 * total], refs[2 * total]

        def copy(j, i):
            here = pl.ds(i * block, block)
            ends = (hbm[j].at[here], vmem[j].at[here])
            return pltpu.make_async_copy(*(ends if j < inputs else ends[::-1]), sems.at[j, i])

        @pl.loop(0, steps)
        def _(i):
            for j in range(inputs):
                copy(j, i).start()

        @pl.loop(0, steps)
        def _(i):
            for j in range(inputs):
                copy(j, i).wait()

            @pl.loop(0, block // unit)
            def _(k):
                here = pl.ds(pl.multiple_of(i * block + k * unit, unit), unit)
                for j, part in enumerate(formula(*(v[here] for v in vmem[:inputs]))):
                    vmem[inputs + j][here] = part

            for j in range(inputs, total):
                copy(j, i).start()

        @pl.loop(0, steps)
        def _(i):
            for j in range(inputs, total):
                copy(j, i).wait()

    return pl.pallas_call(
        kernel,
        in_specs=[pl.BlockSpec(memory_space=pl.ANY)] * inputs,
        out_specs=[pl.BlockSpec(memory_space=pl.ANY)] * count,
        out_shape=[jax.ShapeDtypeStruct((rows, width), bf16)] * count,
        scratch_shapes=[pltpu.VMEM((rows, width), bf16)] * total + [pltpu.SemaphoreType.DMA((total, steps))],
        name="streamed",
    )(*sources)


def copied(sources, sizes):
    width, rows = sources[0].shape[1], sum(sizes)

    def places(heights):
        return [(side, row) for side, n in enumerate(heights) for row in range(n)]

    begin, end = places([s.shape[0] for s in sources]), places(sizes)
    cuts = sorted({0, rows, *range(0, rows, 512)} | {r for r in range(rows) if 0 in (begin[r][1], end[r][1])})
    moves = [(begin[r], end[r], r, n - r) for r, n in zip(cuts, cuts[1:])]

    def kernel(*refs):
        inputs, outs, (held, loaded, stored) = refs[: len(sources)], refs[len(sources) : -3], refs[-3:]
        loads, stores = [], []
        for j, ((s, i), (d, o), r, n) in enumerate(moves):
            here = held.at[pl.ds(r, n)]
            loads.append(pltpu.make_async_copy(inputs[s].at[pl.ds(i, n)], here, loaded.at[j]))
            stores.append(pltpu.make_async_copy(here, outs[d].at[pl.ds(o, n)], stored.at[j]))
        for load in loads:
            load.start()
        for load, store in zip(loads, stores):
            load.wait()
            store.start()
        for store in stores:
            store.wait()

    return pl.pallas_call(
        kernel,
        in_specs=[pl.BlockSpec(memory_space=pl.ANY)] * len(sources),
        out_specs=[pl.BlockSpec(memory_space=pl.ANY)] * len(sizes),
        out_shape=[jax.ShapeDtypeStruct((n, width), bf16) for n in sizes],
        scratch_shapes=[pltpu.VMEM((rows, width), bf16)] + [pltpu.SemaphoreType.DMA((len(moves),))] * 2,
        name="copied",
    )(*sources)


def coordinates(i):
    at = []
    for size in reversed(SIZES):
        at.append(i % size)
        i //= size
    return at[::-1]


def node_at(at):
    i = 0
    for a, size in zip(at, SIZES):
        i = i * size + a % size
    return i


def shifted(i, axis, steps):
    at = coordinates(i)
    at[NODE.index(axis)] += steps
    return node_at(at)


def routed(x, target):
    return lax.ppermute(x, NODE, [(i, target(i)) for i in range(256)])


def ring_sum(v, axis):
    def step(_, carry):
        moving, total = carry
        moving = routed(moving, lambda i: shifted(i, axis, -1))
        return moving, total + moving

    return lax.fori_loop(1, SIZES[NODE.index(axis)], step, (v, v))[1]


def sum_over(v, axes):
    for axis in axes:
        v = lax.psum(v, axis)
    return v


def form_sent(tracked, near, weights):
    tracker = 0.5 * (tracked.astype(f32) + near.astype(f32))
    return ((weights.astype(f32) - step_rate * tracker).astype(bf16),)


def kept(tracked, near, residue):
    return ((residue.astype(f32) + 0.5 * (near.astype(f32) - tracked.astype(f32))).astype(bf16),)


def mixed(own_sent, sent):
    return ((0.5 * (own_sent.astype(f32) + sent.astype(f32))).astype(bf16),)


def both(tracked, near, weights, peer_weights, residue):
    (own_sent,), (sent,) = form_sent(tracked, near, weights), form_sent(near, tracked, peer_weights)
    return *mixed(own_sent, sent), *kept(tracked, near, residue)


def first_sum(level, v):
    if level > 5:
        return sum_over(v, ("y", "x", "core"))
    return ring_sum(v, "z") if level > 0 else lax.psum(ring_sum(v, "x"), "core")


def second_sum(level, v):
    if level > 5:
        return lax.psum(v, "z")
    if level > 2:
        return sum_over(v, ("y", "core", "x"))
    return sum_over(ring_sum(v, "x"), ("core", "y")) if level > 0 else sum_over(v, ("y", "z"))


def flat(x):
    return x.reshape(-1, x.shape[-1])


def after(x, *others):
    return lax.optimization_barrier((x, *others))[0]


def bring(level, x):
    ahead = lambda i: (i + 2**level) % 256
    if level != 6:
        return routed(x, ahead), lambda v: v
    large, small = copied([x], (CUT, x.shape[0] - CUT))
    three_down = lambda i: shifted(i, "z", -3)
    hop = routed(small, three_down)
    near = routed(large, ahead)
    return (near, hop), lambda pair, v: copied([pair[0], routed(after(pair[1], v), three_down)], (x.shape[0],))[0]


def bring_tracked(level, tracked, squares):
    near, finish = bring(level, tracked)
    total = first_sum(level, squares)
    return (finish(near, total) if level == 6 else near), total


def bring_sent(level, own_sent, total, tracked, near, residue):
    sent, finish = bring(level, own_sent)
    (new_residue,) = streamed(kept, (tracked, near, residue), 1, 32)
    if level == 6:
        sent = finish(sent, new_residue)
    total = second_sum(level, after(total, new_residue))
    return sent, new_residue, total


def round_of(level, ids, tok, cot, weights, residue):
    tracked, squares = gradient_call(ids, tok, cot, weights, residue)
    branches = range(LEVELS - 1)
    near, total = lax.switch(level, [partial(bring_tracked, k) for k in branches], tracked, squares)
    (own_sent,) = streamed(form_sent, (tracked, near, flat(weights)), 1)
    sent, new_residue, total = lax.switch(
        level, [partial(bring_sent, k) for k in branches], own_sent, total, tracked, near, flat(residue)
    )
    (new_weights,) = streamed(mixed, (own_sent, sent), 1)
    return new_weights, new_residue, total


def halfway_round(ids, tok, cot, weights, residue):
    ahead = lambda i: (i + 128) % 256
    peer_weights = routed(flat(weights), ahead)
    tracked, squares = gradient_call(ids, tok, cot, weights, residue, looped=True)
    near = routed(tracked, ahead)
    total = sum_over(squares, ("y", "x", "core", "z"))
    new_weights, new_residue = streamed(both, (tracked, near, flat(weights), peer_weights, flat(residue)), 2)
    return new_weights, new_residue, total


def per_device(round_index, sample_ids, token_pool, cotangent_pool, weights, residue):
    level = round_index[0] % LEVELS
    new_weights, new_residue, total = lax.cond(
        level == LEVELS - 1,
        halfway_round,
        partial(round_of, jnp.minimum(level, LEVELS - 2)),
        sample_ids[0],
        token_pool[0],
        cotangent_pool[0],
        weights[0],
        residue[0],
    )
    grad_rms = jnp.sqrt(total.reshape(()) / (256 * weights.size))
    return new_weights.reshape(weights.shape), new_residue.reshape(weights.shape), grad_rms


def solution(mesh):
    torus = Mesh(mesh.devices.reshape(SIZES), NODE)
    split = P(NODE, None, None, None)
    return jax.shard_map(
        per_device,
        mesh=torus,
        in_specs=(P(), P(NODE, None), split, split, split, split),
        out_specs=(split, split, P()),
        check_vma=False,
    )
```

```python
from functools import partial

import jax
import jax.numpy as jnp
from jax import lax
from jax.experimental import pallas as pl
from jax.experimental.pallas import tpu as pltpu
from jax.sharding import Mesh
from jax.sharding import PartitionSpec as P

NODE = ("z", "x", "y", "core")
SIZES = (8, 4, 4, 2)
LEVELS = 8
CUT = 1568
step_rate = 0.1

epsilon = 1e-06
PARTS = (2048,)
bf16, f32 = jnp.bfloat16, jnp.float32


def dot(a, b, ca, cb):
    return lax.dot_general(a, b, (((ca,), (cb,)), ((), ())), preferred_element_type=f32)


def gradient_kernel(looped, ids, tok, cot, w, res, out0, sq, wbuf, rbuf, tbuf, tokb, cotb, proj, grads, sem_in, sem_r, sem_out):
    images, seq, width = tok.shape
    rows = images * seq
    group, head = 256, 64
    outs = (out0,)
    scale = width**-0.5
    loads = [pltpu.make_async_copy(tok, tokb, sem_in.at[0]), pltpu.make_async_copy(cot, cotb, sem_in.at[1])]
    wloads = [pltpu.make_async_copy(w.at[m], wbuf.at[m], sem_in.at[2 + m]) for m in range(4)]
    rloads = [pltpu.make_async_copy(res.at[m], rbuf.at[m], sem_r.at[m]) for m in range(4)]
    pieces, row = [], 0
    for out in outs:
        start, end = row, row + out.shape[0]
        while row < end:
            m, at = divmod(row, width)
            size = min(end - row, width - at)
            pieces.append((pl.ds(at, size), out.at[pl.ds(row - start, size)], m))
            row += size
    stores = [pltpu.make_async_copy(tbuf.at[m, r], o, sem_out.at[j]) for j, (r, o, m) in enumerate(pieces)]
    for c in (loads[0], wloads[0], wloads[1], loads[1], wloads[3], wloads[2], *rloads):
        c.start()

    count = [jnp.int32(0)] * images
    for j in range(ids.shape[0]):
        for b in range(images):
            count[b] = count[b] + (ids[j] == b).astype(jnp.int32)
    count = [c.astype(f32) for c in count]

    loads[0].wait()
    values = tokb[...].reshape(rows, width).astype(f32)
    centered = values - jnp.mean(values, -1, keepdims=True)
    variance = jnp.mean(centered * centered, -1, keepdims=True)
    normed = (centered * lax.rsqrt(variance + epsilon)).astype(bf16)
    for m, extra in ((0, head**-0.5), (1, 1.0), (2, 1.0)):
        wloads[m].wait()
        proj[m] = (dot(normed, wbuf[m], 1, 0) * scale).astype(bf16) * bf16(extra)
    loads[1].wait()
    wloads[3].wait()
    grad_rows = cotb[...].reshape(rows, width)
    proj[3] = (dot(grad_rows, wbuf[3], 1, 1) * scale).astype(bf16)

    heads = group // head
    same = (
        lax.broadcasted_iota(jnp.int32, (heads * seq, group), 0) // seq
        == lax.broadcasted_iota(jnp.int32, (heads * seq, group), 1) // head
    )
    own = same.astype(f32).astype(bf16)
    lane_head = lax.broadcasted_iota(jnp.int32, (seq, group), 1) // head

    def diagonal(x):
        out = x[:seq]
        for h in range(1, heads):
            out = jnp.where(lane_head == h, x[h * seq : (h + 1) * seq], out)
        return out

    def attend(b, share):
        r = pl.ds(b * seq if isinstance(b, int) else pl.multiple_of(b * seq, seq), seq)
        for g in range(width // group):
            c = slice(g * group, (g + 1) * group)
            q, k, v, d = (proj[m, r, c] for m in range(4))
            qs = jnp.concatenate([q] * heads, 0) * own
            ds = jnp.concatenate([d] * heads, 0) * own
            s = dot(k, qs, 1, 1)
            e = jnp.exp(s - jnp.max(s, 0, keepdims=True))
            p = e * (1.0 / jnp.sum(e, 0, keepdims=True))
            ph = p.astype(bf16)
            dp = dot(v, ds, 1, 1)
            sg = (p * (dp - jnp.sum(dp * p, 0, keepdims=True)) * share).astype(bf16)
            grads[2, r, c] = (dot(ph, ds, 1, 0) * share).astype(bf16)
            grads[1, r, c] = dot(sg, qs, 1, 0).astype(bf16)
            grads[3, r, c] = (diagonal(dot(ph, v, 0, 0)) * share).astype(bf16)
            grads[0, r, c] = (diagonal(dot(sg, k, 0, 0)) * head**-0.5).astype(bf16)

    if looped:

        @pl.loop(0, images)
        def _(b):
            share = jnp.int32(0)
            for j in range(ids.shape[0]):
                share = share + (ids[j] == b).astype(jnp.int32)
            attend(b, share.astype(f32))

    else:
        for b in range(images):
            attend(b, count[b])

    total = jnp.zeros((8, width), f32)
    for m in range(4):
        left, right = (grads[3], grad_rows) if m == 3 else (normed, grads[m])
        gradient = dot(left, right, 0, 0) * scale
        rloads[m].wait()
        tbuf[m] = (rbuf[m].astype(f32) + gradient).astype(bf16)
        for store, piece in zip(stores, pieces):
            if piece[2] == m:
                store.start()
        total = total + jnp.sum((gradient * gradient).reshape(-1, 8, width), 0)
    sq[0] = jnp.sum(total)
    for store in stores:
        store.wait()


def gradient_call(ids, tok, cot, w, res, looped=False):
    images, seq, width = tok.shape
    rows = images * seq
    hbm = pl.BlockSpec(memory_space=pl.ANY)
    smem = pl.BlockSpec(memory_space=pltpu.SMEM)
    return pl.pallas_call(
        partial(gradient_kernel, looped),
        in_specs=[smem, hbm, hbm, hbm, hbm],
        out_specs=[hbm, smem],
        out_shape=[jax.ShapeDtypeStruct((n, width), bf16) for n in PARTS] + [jax.ShapeDtypeStruct((1,), f32)],
        scratch_shapes=[
            pltpu.VMEM((4, width, width), bf16),
            pltpu.VMEM((4, width, width), bf16),
            pltpu.VMEM((4, width, width), bf16),
            pltpu.VMEM((images, seq, width), bf16),
            pltpu.VMEM((images, seq, width), bf16),
            pltpu.VMEM((4, rows, width), bf16),
            pltpu.VMEM((4, rows, width), bf16),
            pltpu.SemaphoreType.DMA((6,)),
            pltpu.SemaphoreType.DMA((4,)),
            pltpu.SemaphoreType.DMA((4,)),
        ],
        name="gradient",
    )(ids, tok, cot, w, res)


def streamed(formula, sources, count, unit=128, block=256):
    rows, width = sources[0].shape
    steps, inputs, total = rows // block, len(sources), len(sources) + count

    def kernel(*refs):
        hbm, vmem, sems = refs[:total], refs[total : 2 * total], refs[2 * total]

        def copy(j, i):
            here = pl.ds(i * block, block)
            ends = (hbm[j].at[here], vmem[j].at[here])
            return pltpu.make_async_copy(*(ends if j < inputs else ends[::-1]), sems.at[j, i])

        @pl.loop(0, steps)
        def _(i):
            for j in range(inputs):
                copy(j, i).start()

        @pl.loop(0, steps)
        def _(i):
            for j in range(inputs):
                copy(j, i).wait()

            @pl.loop(0, block // unit)
            def _(k):
                here = pl.ds(pl.multiple_of(i * block + k * unit, unit), unit)
                for j, part in enumerate(formula(*(v[here] for v in vmem[:inputs]))):
                    vmem[inputs + j][here] = part

            for j in range(inputs, total):
                copy(j, i).start()

        @pl.loop(0, steps)
        def _(i):
            for j in range(inputs, total):
                copy(j, i).wait()

    return pl.pallas_call(
        kernel,
        in_specs=[pl.BlockSpec(memory_space=pl.ANY)] * inputs,
        out_specs=[pl.BlockSpec(memory_space=pl.ANY)] * count,
        out_shape=[jax.ShapeDtypeStruct((rows, width), bf16)] * count,
        scratch_shapes=[pltpu.VMEM((rows, width), bf16)] * total + [pltpu.SemaphoreType.DMA((total, steps))],
        name="streamed",
    )(*sources)


def copied(sources, sizes):
    width, rows = sources[0].shape[1], sum(sizes)

    def places(heights):
        return [(side, row) for side, n in enumerate(heights) for row in range(n)]

    begin, end = places([s.shape[0] for s in sources]), places(sizes)
    cuts = sorted({0, rows, *range(0, rows, 512)} | {r for r in range(rows) if 0 in (begin[r][1], end[r][1])})
    moves = [(begin[r], end[r], r, n - r) for r, n in zip(cuts, cuts[1:])]

    def kernel(*refs):
        inputs, outs, (held, loaded, stored) = refs[: len(sources)], refs[len(sources) : -3], refs[-3:]
        loads, stores = [], []
        for j, ((s, i), (d, o), r, n) in enumerate(moves):
            here = held.at[pl.ds(r, n)]
            loads.append(pltpu.make_async_copy(inputs[s].at[pl.ds(i, n)], here, loaded.at[j]))
            stores.append(pltpu.make_async_copy(here, outs[d].at[pl.ds(o, n)], stored.at[j]))
        for load in loads:
            load.start()
        for load, store in zip(loads, stores):
            load.wait()
            store.start()
        for store in stores:
            store.wait()

    return pl.pallas_call(
        kernel,
        in_specs=[pl.BlockSpec(memory_space=pl.ANY)] * len(sources),
        out_specs=[pl.BlockSpec(memory_space=pl.ANY)] * len(sizes),
        out_shape=[jax.ShapeDtypeStruct((n, width), bf16) for n in sizes],
        scratch_shapes=[pltpu.VMEM((rows, width), bf16)] + [pltpu.SemaphoreType.DMA((len(moves),))] * 2,
        name="copied",
    )(*sources)


def coordinates(i):
    at = []
    for size in reversed(SIZES):
        at.append(i % size)
        i //= size
    return at[::-1]


def node_at(at):
    i = 0
    for a, size in zip(at, SIZES):
        i = i * size + a % size
    return i


def shifted(i, axis, steps):
    at = coordinates(i)
    at[NODE.index(axis)] += steps
    return node_at(at)


def routed(x, target):
    return lax.ppermute(x, NODE, [(i, target(i)) for i in range(256)])


def ring_sum(v, axis):
    def step(_, carry):
        moving, total = carry
        moving = routed(moving, lambda i: shifted(i, axis, -1))
        return moving, total + moving

    return lax.fori_loop(1, SIZES[NODE.index(axis)], step, (v, v))[1]


def sum_over(v, axes):
    for axis in axes:
        v = lax.psum(v, axis)
    return v


def form_sent(tracked, near, weights):
    tracker = 0.5 * (tracked.astype(f32) + near.astype(f32))
    return ((weights.astype(f32) - step_rate * tracker).astype(bf16),)


def kept(tracked, near, residue):
    return ((residue.astype(f32) + 0.5 * (near.astype(f32) - tracked.astype(f32))).astype(bf16),)


def mixed(own_sent, sent):
    return ((0.5 * (own_sent.astype(f32) + sent.astype(f32))).astype(bf16),)


def both(tracked, near, weights, peer_weights, residue):
    (own_sent,), (sent,) = form_sent(tracked, near, weights), form_sent(near, tracked, peer_weights)
    return *mixed(own_sent, sent), *kept(tracked, near, residue)


def first_sum(level, v):
    if level > 5:
        return sum_over(v, ("y", "x", "core"))
    return ring_sum(v, "z") if level > 0 else lax.psum(ring_sum(v, "x"), "core")


def second_sum(level, v):
    if level > 5:
        return lax.psum(v, "z")
    if level > 2:
        v = sum_over(v, ("y", "core"))
        return ring_sum(v, "x") if level == 3 else lax.psum(v, "x")
    if level == 0:
        return sum_over(v, ("y", "z"))
    v = lax.psum(ring_sum(v, "x"), "core")
    return ring_sum(v, "y") if level == 1 else lax.psum(v, "y")


def flat(x):
    return x.reshape(-1, x.shape[-1])


def after(x, *others):
    return lax.optimization_barrier((x, *others))[0]


def bring(level, x):
    ahead = lambda i: (i + 2**level) % 256
    if level != 6:
        return routed(x, ahead), lambda v: v
    large, small = copied([x], (CUT, x.shape[0] - CUT))
    three_down = lambda i: shifted(i, "z", -3)
    hop = routed(small, three_down)
    near = routed(large, ahead)
    return (near, hop), lambda pair, v: copied([pair[0], routed(after(pair[1], v), three_down)], (x.shape[0],))[0]


def bring_tracked(level, tracked, squares):
    near, finish = bring(level, tracked)
    total = first_sum(level, squares)
    return (finish(near, total) if level == 6 else near), total


def bring_sent(level, own_sent, total, tracked, near, residue):
    sent, finish = bring(level, own_sent)
    (new_residue,) = streamed(kept, (tracked, near, residue), 1, 32)
    if level == 6:
        sent = finish(sent, new_residue)
    total = second_sum(level, after(total, new_residue))
    return sent, new_residue, total


def round_of(level, ids, tok, cot, weights, residue):
    tracked, squares = gradient_call(ids, tok, cot, weights, residue)
    branches = range(LEVELS - 1)
    near, total = lax.switch(level, [partial(bring_tracked, k) for k in branches], tracked, squares)
    (own_sent,) = streamed(form_sent, (tracked, near, flat(weights)), 1)
    sent, new_residue, total = lax.switch(
        level, [partial(bring_sent, k) for k in branches], own_sent, total, tracked, near, flat(residue)
    )
    (new_weights,) = streamed(mixed, (own_sent, sent), 1)
    return new_weights, new_residue, total


def halfway_round(ids, tok, cot, weights, residue):
    ahead = lambda i: (i + 128) % 256
    peer_weights = routed(flat(weights), ahead)
    tracked, squares = gradient_call(ids, tok, cot, weights, residue, looped=True)
    near = routed(tracked, ahead)
    total = sum_over(squares, ("y", "x", "core", "z"))
    new_weights, new_residue = streamed(both, (tracked, near, flat(weights), peer_weights, flat(residue)), 2)
    return new_weights, new_residue, total


def per_device(round_index, sample_ids, token_pool, cotangent_pool, weights, residue):
    level = round_index[0] % LEVELS
    new_weights, new_residue, total = lax.cond(
        level == LEVELS - 1,
        halfway_round,
        partial(round_of, jnp.minimum(level, LEVELS - 2)),
        sample_ids[0],
        token_pool[0],
        cotangent_pool[0],
        weights[0],
        residue[0],
    )
    grad_rms = jnp.sqrt(total.reshape(()) / (256 * weights.size))
    return new_weights.reshape(weights.shape), new_residue.reshape(weights.shape), grad_rms


def solution(mesh):
    torus = Mesh(mesh.devices.reshape(SIZES), NODE)
    split = P(NODE, None, None, None)
    return jax.shard_map(
        per_device,
        mesh=torus,
        in_specs=(P(), P(NODE, None), split, split, split, split),
        out_specs=(split, split, P()),
        check_vma=False,
    )
```
